16 devices in a mesh: stage: 2 (over y, z), data: 8 (over x, core).
Axes of the slice: x: 4, y: 2, z: 1, core: 2. Of those that a mesh axis runs over, the one named last changes fastest.
The devices are a block of a 4x4x8 slice.
Arguments:
- w_master: float32 [48, 2048, 1024], P('stage', 'data'), parts along dimension 0
- momentum: float32 [48, 2048, 1024], P('stage', 'data'), parts along dimension 0
- grad: bfloat16 [48, 2048, 1024], P('stage', 'data'), parts along dimension 0
Outputs:
- output 1: bfloat16 [48, 2048, 1024], P('stage'), parts along dimension 0
- output 2: float32 [48, 2048, 1024], P('stage', 'data'), parts along dimension 0
There are 2 independent parts. The reference program is written for one: setup_inputs(seed, part) draws one part's arguments, and reference() takes and returns one part's arrays. A program takes and returns all parts, laid end to end along the dimension named above; each array names one.
All inputs are finite; a program needn't handle non-finite values.
Results may differ from the reference program's by a relative error of at most 0.00729924.
Values are sent between devices in bfloat16 or wider.
A program may use at most 768 MiB of HBM per device.

```python
import math
import jax
import jax.numpy as jnp
from jax import lax

DATA_DEVS = 8
MATS_DEV = 3
D = 2048
FF_E = 1024
NS_ITERS = 5

MOMENTUM = 0.95
LEARN_RATE = 0.02
WEIGHT_DECAY = 0.1
NORM_EPS = 1e-7
COEF_A = 3.4445
COEF_B = -4.7750
COEF_C = 2.0315
RMS_SCALE = 0.2 * math.sqrt(max(D, FF_E))


def setup_inputs(seed: int = 0, part: int = 0) -> dict:
    mat_count = MATS_DEV * DATA_DEVS
    key = jax.random.fold_in(jax.random.key(seed), part)
    keys = jax.random.split(key, 7)
    w_master = 0.02 * jax.random.normal(keys[0], (mat_count, D, FF_E), jnp.float32)
    left_fac = jax.random.normal(keys[1], (mat_count, D, 4), jnp.float32)
    right_fac = jax.random.normal(keys[2], (mat_count, 4, FF_E), jnp.float32)
    shared = 0.25 * jnp.einsum("mdr,mrf->mdf", left_fac, right_fac)
    row_scale = jax.random.uniform(keys[3], (mat_count, D, 1), jnp.float32, 0.5, 2.0)
    momentum = row_scale * (jax.random.normal(keys[4], (mat_count, D, FF_E), jnp.float32) + shared)
    grad_scale = jax.random.uniform(keys[5], (mat_count, D, 1), jnp.float32, 0.5, 2.0)
    grad = (grad_scale * jax.random.normal(keys[6], (mat_count, D, FF_E), jnp.float32)).astype(jnp.bfloat16)
    return {"w_master": w_master, "momentum": momentum, "grad": grad}


def newton_schulz(x_mat):
    for iteration in range(NS_ITERS):
        gram_mat = jnp.dot(x_mat, x_mat.T, preferred_element_type=jnp.float32).astype(jnp.bfloat16)
        square = jnp.dot(gram_mat, gram_mat, preferred_element_type=jnp.float32)
        poly_mat = (COEF_B * gram_mat.astype(jnp.float32) + COEF_C * square).astype(jnp.bfloat16)
        prod_mat = jnp.dot(poly_mat, x_mat, preferred_element_type=jnp.float32)
        x_mat = (COEF_A * x_mat.astype(jnp.float32) + prod_mat).astype(jnp.bfloat16)
    return x_mat


def orthogonalize(mom_one):
    frob_norm = jnp.sqrt(jnp.sum(mom_one * mom_one))
    x_mat = (mom_one.astype(jnp.bfloat16).astype(jnp.float32) / (frob_norm + NORM_EPS)).astype(jnp.bfloat16)
    if D > FF_E:
        x_mat = newton_schulz(x_mat.T).T
    else:
        x_mat = newton_schulz(x_mat)
    return x_mat.astype(jnp.float32) * RMS_SCALE


def reference(w_master, momentum, grad):
    mom_new = MOMENTUM * momentum + grad.astype(jnp.float32)

    def update_one(w_and_m):
        w_one, mom_one = w_and_m
        w_new = w_one - LEARN_RATE * (orthogonalize(mom_one) + WEIGHT_DECAY * w_one)
        return w_new.astype(jnp.bfloat16)

    params = lax.map(update_one, (w_master, mom_new))
    return params, mom_new
```

```python
import functools
import math

import jax
import jax.numpy as jnp
from jax import lax
from jax.experimental import pallas as pl
from jax.experimental.pallas import tpu as pltpu
from jax.sharding import PartitionSpec as P

NS_ITERS = 5
MOMENTUM = 0.95
LEARN_RATE = 0.02
WEIGHT_DECAY = 0.1
NORM_EPS = 1e-7
COEF_A = 3.4445
COEF_B = -4.7750
COEF_C = 2.0315

MESH = pl.DeviceIdType.MESH
CORES = 2
BLK = 256
CHUNK = 32
VMEM_LIMIT = 60 * 1024 * 1024
F32 = jnp.float32
BF16 = jnp.bfloat16


def aligned(start, size):
    return pl.ds(pl.multiple_of(start, size), size)


def step_offsets(k, chips):
    return lax.rem(k // CORES + 1, chips), lax.rem(k, CORES)


def target_of(me, k, chips):
    dx, dc = step_offsets(k, chips)
    return lax.rem(me // CORES + dx, chips) * CORES + lax.rem(lax.rem(me, CORES) + dc, CORES)


def source_of(me, k, chips):
    dx, dc = step_offsets(k, chips)
    return lax.rem(me // CORES + chips - dx, chips) * CORES + lax.rem(lax.rem(me, CORES) + dc, CORES)


def greet_group(me, group, chips):
    barrier = pltpu.get_barrier_semaphore()
    for k in range(group):
        if k != group - CORES:
            pl.semaphore_signal(barrier, inc=1, device_id={"data": target_of(me, k, chips)}, device_id_type=MESH)
    pl.semaphore_wait(barrier, group - 1)


def newton_schulz(y, gram, poly):
    rows, cols = y.shape

    def iteration(_, carry):
        def gram_block(i, c):
            at = aligned(i * BLK, BLK)
            gram[at, :] = lax.dot_general(y[:, at], y[...], (((0,), (0,)), ((), ())), preferred_element_type=F32).astype(BF16)
            return c

        def poly_block(i, c):
            at = aligned(i * BLK, BLK)
            part = gram[at, :]
            square = jnp.dot(part, gram[...], preferred_element_type=F32)
            poly[at, :] = (COEF_B * part.astype(F32) + COEF_C * square).astype(BF16)
            return c

        def update_block(i, c):
            at = aligned(i * BLK, BLK)
            part = y[at, :]
            prod = jnp.dot(part, poly[...], preferred_element_type=F32)
            y[at, :] = (COEF_A * part.astype(F32) + prod).astype(BF16)
            return c

        lax.fori_loop(0, cols // BLK, gram_block, 0)
        lax.fori_loop(0, cols // BLK, poly_block, 0)
        lax.fori_loop(0, rows // BLK, update_block, 0)
        return carry

    lax.fori_loop(0, NS_ITERS, iteration, 0)


def start_weights(me, wave, group, w_hbm, w_vmem, w_sem, chips):
    def load(k, c):
        owner = source_of(me, k, chips)
        pltpu.make_async_copy(w_hbm.at[wave * group + owner], w_vmem.at[k], w_sem.at[k]).start()
        return c

    lax.fori_loop(0, group, load, 0)


def orthogonalize_wave(me, wave, group, chips, land, norms, w_hbm, w_out, y, gram, poly, norm_v, x_land, w_vmem, o_vmem,
                       y_sem, x_send, x_recv, w_sem, o_sem):
    rows, cols = y.shape
    rows_dev = rows // group
    own_k = group - CORES
    scale = 0.2 * math.sqrt(max(rows, cols))

    load_y = pltpu.make_async_copy(land.at[wave], y, y_sem.at[0])
    load_n = pltpu.make_async_copy(norms.at[wave], norm_v, y_sem.at[1])
    load_y.start()
    load_n.start()
    load_y.wait()
    load_n.wait()
    total = jnp.sum(jnp.sum(norm_v[...], axis=0), axis=(0, 1), keepdims=True)
    denom = jnp.sqrt(total) + NORM_EPS

    def normalise(i, c):
        at = aligned(i * CHUNK, CHUNK)
        y[at, :] = (y[at, :].astype(F32) / denom).astype(BF16)
        return c

    lax.fori_loop(0, rows // CHUNK, normalise, 0)
    newton_schulz(y, gram, poly)

    def row_copy(k):
        target = target_of(me, k, chips)
        return pltpu.make_async_remote_copy(
            src_ref=y.at[aligned(target * rows_dev, rows_dev)],
            dst_ref=x_land.at[k],
            send_sem=x_send.at[k],
            recv_sem=x_recv.at[k],
            device_id={"data": target},
            device_id_type=MESH,
        )

    for k in range(group):
        if k != own_k:
            row_copy(k).start()
    own = pltpu.make_async_copy(y.at[aligned(me * rows_dev, rows_dev)], x_land.at[own_k], y_sem.at[0])
    own.start()

    def update(j, c):
        k = lax.rem(j + own_k, group)
        owner = source_of(me, k, chips)
        pltpu.make_async_copy(w_hbm.at[wave * group + owner], w_vmem.at[k], w_sem.at[k]).wait()

        @pl.when(k == own_k)
        def _():
            own.wait()

        @pl.when(k != own_k)
        def _():
            row_copy(k).wait_recv()

        def chunk(i, c2):
            at = aligned(i * CHUNK, CHUNK)
            w_old = w_vmem[k, at, :]
            ortho = x_land[k, at, :].astype(F32) * scale
            o_vmem[k, at, :] = (w_old - LEARN_RATE * (ortho + WEIGHT_DECAY * w_old)).astype(BF16)
            return c2

        lax.fori_loop(0, rows_dev // CHUNK, chunk, 0)
        pltpu.make_async_copy(o_vmem.at[k], w_out.at[owner], o_sem.at[k]).start()
        return c

    lax.fori_loop(0, group, update, 0)

    def finish(k, c):
        owner = source_of(me, k, chips)
        pltpu.make_async_copy(o_vmem.at[k], w_out.at[owner], o_sem.at[k]).wait()

        @pl.when(k != own_k)
        def _():
            row_copy(k).wait_send()

        return c

    lax.fori_loop(0, group, finish, 0)


def first_kernel(group, waves, mom, grad, w_hbm, w_out, land, norms, send, norm_send, mom_v, grad_v, load_sem, m_send, m_recv,
                 n_send, n_recv, l_sem, *work):
    me = lax.axis_index("data")
    chips = group // CORES
    own_k = group - CORES
    rows_dev, cols = mom.shape[1:]
    steps = waves * group
    greet_group(me, group, chips)
    y, gram, poly, norm_v, x_land, w_vmem, o_vmem, y_sem, x_send, x_recv, w_sem, o_sem = work
    mine = aligned(me * rows_dev, rows_dev)

    def loads(t):
        wave, k = t // group, lax.rem(t, group)
        mat = wave * group + target_of(me, k, chips)
        slot = lax.rem(t, 2)
        return (
            pltpu.make_async_copy(mom.at[mat], mom_v.at[slot], load_sem.at[0, slot]),
            pltpu.make_async_copy(grad.at[mat], grad_v.at[slot], load_sem.at[1, slot]),
        )

    def remote(wave, k):
        target = target_of(me, k, chips)
        t = wave * group + k
        rows = pltpu.make_async_remote_copy(
            src_ref=send.at[t], dst_ref=land.at[wave, mine], send_sem=m_send.at[wave, k], recv_sem=m_recv.at[wave, k],
            device_id={"data": target}, device_id_type=MESH)
        norm = pltpu.make_async_remote_copy(
            src_ref=norm_send.at[t], dst_ref=norms.at[wave, me], send_sem=n_send.at[wave, k], recv_sem=n_recv.at[wave, k],
            device_id={"data": target}, device_id_type=MESH)
        return rows, norm

    def local(wave):
        t = wave * group + own_k
        return (
            pltpu.make_async_copy(send.at[t], land.at[wave, mine], l_sem.at[0, wave]),
            pltpu.make_async_copy(norm_send.at[t], norms.at[wave, me], l_sem.at[1, wave]),
        )

    def dispatch(t):
        wave, k = t // group, lax.rem(t, group)

        @pl.when(k == own_k)
        def _():
            for copy in local(wave):
                copy.start()

        @pl.when(k != own_k)
        def _():
            for copy in remote(wave, k):
                copy.start()

    for copy in loads(0):
        copy.start()

    def form(t, c):
        @pl.when(t + 1 < steps)
        def _():
            for copy in loads(t + 1):
                copy.start()

        for copy in loads(t):
            copy.wait()
        slot = lax.rem(t, 2)

        def chunk(i, acc):
            at = aligned(i * CHUNK, CHUNK)
            new = MOMENTUM * mom_v[slot, at, :] + grad_v[slot, at, :].astype(F32)
            send[t, at, :] = new.astype(BF16)
            sq = new * new
            for r in range(0, CHUNK, 8):
                acc = acc + sq[r:r + 8, :]
            return acc

        acc = lax.fori_loop(0, rows_dev // CHUNK, chunk, jnp.zeros((8, cols), F32))
        part = acc[:, 0:128]
        for col in range(128, cols, 128):
            part = part + acc[:, col:col + 128]
        norm_send[t] = part

        @pl.when(t > 0)
        def _():
            dispatch(t - 1)

        return c

    lax.fori_loop(0, steps, form, 0)
    dispatch(jnp.int32(steps - 1))
    start_weights(me, 0, group, w_hbm, w_vmem, w_sem, chips)

    def arrived(wave):
        for k in range(group):
            if k != own_k:
                for copy in remote(wave, k):
                    copy.wait_recv()
        for copy in local(wave):
            copy.wait()

    arrived(0)
    orthogonalize_wave(me, 0, group, chips, land, norms, w_hbm, w_out, *work)
    for wave in range(1, waves):
        arrived(wave)
    for wave in range(waves):
        for k in range(group):
            if k != own_k:
                for copy in remote(wave, k):
                    copy.wait_send()


def later_kernel(group, wave, land, norms, w_hbm, w_out, *work):
    me = lax.axis_index("data")
    chips = group // CORES
    greet_group(me, group, chips)
    start_weights(me, wave, group, w_hbm, work[5], work[10], chips)
    orthogonalize_wave(me, wave, group, chips, land, norms, w_hbm, w_out, *work)


def momentum_kernel(mom, grad, _, out):
    out[...] = MOMENTUM * mom[...] + grad[...].astype(F32)


def place_kernel(src, *refs):
    refs[-1][...] = src[0]


def solution(mesh):
    group = mesh.shape["data"]
    row_spec = P("stage", "data", None)
    full_spec = P("stage", None, None)
    any_spec = pl.BlockSpec(memory_space=pl.ANY)

    def local_step(w_rows, mom_rows, grad_rows):
        mats, rows_dev, cols = mom_rows.shape
        rows = rows_dev * group
        waves = mats // group
        ns_flops = NS_ITERS * 2 * (2 * rows * cols * cols + cols**3)
        work = [
            pltpu.VMEM((rows, cols), BF16),
            pltpu.VMEM((cols, cols), BF16),
            pltpu.VMEM((cols, cols), BF16),
            pltpu.VMEM((group, 8, 128), F32),
            pltpu.VMEM((group, rows_dev, cols), BF16),
            pltpu.VMEM((group, rows_dev, cols), F32),
            pltpu.VMEM((group, rows_dev, cols), BF16),
            pltpu.SemaphoreType.DMA((2,)),
            pltpu.SemaphoreType.DMA((group,)),
            pltpu.SemaphoreType.DMA((group,)),
            pltpu.SemaphoreType.DMA((group,)),
            pltpu.SemaphoreType.DMA((group,)),
        ]
        w_new_shape = jax.ShapeDtypeStruct((group, rows_dev, cols), BF16)
        cost = pl.CostEstimate(flops=ns_flops, bytes_accessed=8 * rows * cols, transcendentals=0)
        w_new, land, norms = pl.pallas_call(
            functools.partial(first_kernel, group, waves),
            name="first_wave",
            out_shape=(
                w_new_shape,
                jax.ShapeDtypeStruct((waves, rows, cols), BF16),
                jax.ShapeDtypeStruct((waves, group, 8, 128), F32),
            ),
            in_specs=[any_spec] * 3,
            out_specs=(any_spec,) * 3,
            scratch_shapes=[
                pltpu.VMEM((mats, rows_dev, cols), BF16),
                pltpu.VMEM((mats, 8, 128), F32),
                pltpu.VMEM((2, rows_dev, cols), F32),
                pltpu.VMEM((2, rows_dev, cols), BF16),
                pltpu.SemaphoreType.DMA((2, 2)),
                pltpu.SemaphoreType.DMA((waves, group)),
                pltpu.SemaphoreType.DMA((waves, group)),
                pltpu.SemaphoreType.DMA((waves, group)),
                pltpu.SemaphoreType.DMA((waves, group)),
                pltpu.SemaphoreType.DMA((2, waves)),
                *work,
            ],
            compiler_params=pltpu.CompilerParams(collective_id=0, has_side_effects=True, vmem_limit_bytes=VMEM_LIMIT),
            cost_estimate=cost,
        )(mom_rows, grad_rows, w_rows)
        gathered = [lax.all_gather(w_new, "data", axis=0)]
        for wave in range(1, waves):
            w_new = pl.pallas_call(
                functools.partial(later_kernel, group, wave),
                name=f"wave_{wave}",
                out_shape=w_new_shape,
                in_specs=[any_spec] * 3,
                out_specs=any_spec,
                scratch_shapes=work,
                compiler_params=pltpu.CompilerParams(collective_id=wave, has_side_effects=True, vmem_limit_bytes=VMEM_LIMIT),
                cost_estimate=cost,
            )(land, norms, w_rows)
            gathered.append(lax.all_gather(w_new, "data", axis=0))
        mom_new = pl.pallas_call(
            momentum_kernel,
            name="momentum",
            grid=(mats,),
            out_shape=jax.ShapeDtypeStruct(mom_rows.shape, F32),
            in_specs=[
                pl.BlockSpec((1, rows_dev, cols), lambda i: (i, 0, 0)),
                pl.BlockSpec((1, rows_dev, cols), lambda i: (i, 0, 0)),
                any_spec,
            ],
            out_specs=pl.BlockSpec((1, rows_dev, cols), lambda i: (i, 0, 0)),
            cost_estimate=pl.CostEstimate(flops=mats * rows_dev * cols * 100, bytes_accessed=10 * mats * rows_dev * cols, transcendentals=0),
        )(mom_rows, grad_rows, w_new)
        params = mom_new
        for wave in range(waves):
            params = pl.pallas_call(
                place_kernel,
                name=f"place_{wave}",
                grid=(group, group),
                out_shape=jax.ShapeDtypeStruct((mats, rows, cols), BF16),
                in_specs=[pl.BlockSpec((1, 1, rows_dev, cols), lambda o, d: (d, o, 0, 0)), any_spec],
                out_specs=pl.BlockSpec((1, rows_dev, cols), lambda o, d, wave=wave: (wave * group + o, d, 0)),
                input_output_aliases={1: 0} if wave else {},
                cost_estimate=pl.CostEstimate(flops=group * rows * cols * 40, bytes_accessed=4 * group * rows * cols, transcendentals=0),
            )(gathered[wave], params)
        return params, mom_new

    return jax.shard_map(local_step, mesh=mesh, in_specs=(row_spec,) * 3, out_specs=(full_spec, row_spec), check_vma=False)
```

```python
import functools
import math

import jax
import jax.numpy as jnp
from jax import lax
from jax.experimental import pallas as pl
from jax.experimental.pallas import tpu as pltpu
from jax.sharding import PartitionSpec as P


NS_ITERS = 5
MOMENTUM = 0.95
LEARN_RATE = 0.02
WEIGHT_DECAY = 0.1
NORM_EPS = 1e-7
COEF_A = 3.4445
COEF_B = -4.7750
COEF_C = 2.0315

MESH = pl.DeviceIdType.MESH
CORES = 2
BLK = 256
CHUNK = 32
SLOTS = 8
VMEM_LIMIT = 67043328
F32 = jnp.float32
BF16 = jnp.bfloat16


def aligned(start, size):
    return pl.ds(pl.multiple_of(start, size), size)


def step_offsets(k, chips):
    return lax.rem(k // CORES + 1, chips), lax.rem(k, CORES)


def target_of(me, k, chips):
    dx, dc = step_offsets(k, chips)
    return lax.rem(me // CORES + dx, chips) * CORES + lax.rem(lax.rem(me, CORES) + dc, CORES)


def source_of(me, k, chips):
    dx, dc = step_offsets(k, chips)
    return lax.rem(me // CORES + chips - dx, chips) * CORES + lax.rem(lax.rem(me, CORES) + dc, CORES)


def greet_group(me, group, chips):
    barrier = pltpu.get_barrier_semaphore()
    for k in range(group):
        if k != group - CORES:
            pl.semaphore_signal(barrier, inc=1, device_id={"data": target_of(me, k, chips)}, device_id_type=MESH)
    pl.semaphore_wait(barrier, group - 1)


def newton_schulz(y, gram, poly):
    rows, cols = y.shape

    def iteration(_, carry):
        def gram_block(i, c):
            at = aligned(i * BLK, BLK)
            gram[at, :] = lax.dot_general(y[:, at], y[...], (((0,), (0,)), ((), ())), preferred_element_type=F32).astype(BF16)
            return c

        def poly_block(i, c):
            at = aligned(i * BLK, BLK)
            part = gram[at, :]
            square = jnp.dot(part, gram[...], preferred_element_type=F32)
            poly[at, :] = (COEF_B * part.astype(F32) + COEF_C * square).astype(BF16)
            return c

        def update_block(i, c):
            at = aligned(i * BLK, BLK)
            part = y[at, :]
            prod = jnp.dot(part, poly[...], preferred_element_type=F32)
            y[at, :] = (COEF_A * part.astype(F32) + prod).astype(BF16)
            return c

        lax.fori_loop(0, cols // BLK, gram_block, 0)
        lax.fori_loop(0, cols // BLK, poly_block, 0)
        lax.fori_loop(0, rows // BLK, update_block, 0)
        return carry

    lax.fori_loop(0, NS_ITERS, iteration, 0)


def start_weights(me, wave, group, w_hbm, w_vmem, w_sem, chips):
    def load(k, c):
        owner = source_of(me, k, chips)
        pltpu.make_async_copy(w_hbm.at[wave * group + owner], w_vmem.at[k], w_sem.at[k]).start()
        return c

    lax.fori_loop(0, group, load, 0)


def iterate(wave, land, norms, y, gram, poly, norm_v, y_sem):
    rows = y.shape[0]
    load_y = pltpu.make_async_copy(land.at[wave], y, y_sem.at[0])
    load_n = pltpu.make_async_copy(norms.at[wave], norm_v, y_sem.at[1])
    load_y.start()
    load_n.start()
    load_y.wait()
    load_n.wait()
    total = jnp.sum(jnp.sum(norm_v[...], axis=0), axis=(0, 1), keepdims=True)
    denom = jnp.sqrt(total) + NORM_EPS

    def normalise(i, c):
        at = aligned(i * CHUNK, CHUNK)
        y[at, :] = (y[at, :].astype(F32) / denom).astype(BF16)
        return c

    lax.fori_loop(0, rows // CHUNK, normalise, 0)
    newton_schulz(y, gram, poly)


def new_rows(scale, w_vmem, x_vmem, o_vmem, k):
    def chunk(i, c):
        at = aligned(i * CHUNK, CHUNK)
        w_old = w_vmem[k, at, :]
        ortho = x_vmem[k, at, :].astype(F32) * scale
        o_vmem[k, at, :] = (w_old - LEARN_RATE * (ortho + WEIGHT_DECAY * w_old)).astype(BF16)
        return c

    lax.fori_loop(0, w_vmem.shape[1] // CHUNK, chunk, 0)


def store_rows(o_vmem, w_lo, w_hi, o_sem, k, owner, act):
    half = w_lo.shape[0]

    @pl.when(owner < half)
    def _():
        act(pltpu.make_async_copy(o_vmem.at[k], w_lo.at[owner], o_sem.at[k]))

    @pl.when(owner >= half)
    def _():
        act(pltpu.make_async_copy(o_vmem.at[k], w_hi.at[owner - half], o_sem.at[k]))


def orthogonalize_wave(me, wave, group, chips, land, norms, w_hbm, w_lo, w_hi, y, gram, poly, norm_v, x_land, w_vmem, o_vmem,
                       y_sem, x_send, x_recv, w_sem, o_sem, then):
    rows, cols = y.shape
    rows_dev = rows // group
    own_k = group - CORES
    scale = 0.2 * math.sqrt(max(rows, cols))
    iterate(wave, land, norms, y, gram, poly, norm_v, y_sem)

    def row_copy(k):
        target = target_of(me, k, chips)
        return pltpu.make_async_remote_copy(
            src_ref=y.at[aligned(target * rows_dev, rows_dev)],
            dst_ref=x_land.at[k],
            send_sem=x_send.at[k],
            recv_sem=x_recv.at[k],
            device_id={"data": target},
            device_id_type=MESH,
        )

    for k in range(group):
        if k != own_k:
            row_copy(k).start()
    then()
    own = pltpu.make_async_copy(y.at[aligned(me * rows_dev, rows_dev)], x_land.at[own_k], y_sem.at[0])
    own.start()

    def update(j, c):
        k = lax.rem(j + own_k, group)
        owner = source_of(me, k, chips)
        pltpu.make_async_copy(w_hbm.at[wave * group + owner], w_vmem.at[k], w_sem.at[k]).wait()

        @pl.when(k == own_k)
        def _():
            own.wait()

        @pl.when(k != own_k)
        def _():
            row_copy(k).wait_recv()

        new_rows(scale, w_vmem, x_land, o_vmem, k)
        store_rows(o_vmem, w_lo, w_hi, o_sem, k, owner, lambda copy: copy.start())
        return c

    lax.fori_loop(0, group, update, 0)

    def finish(k, c):
        owner = source_of(me, k, chips)
        store_rows(o_vmem, w_lo, w_hi, o_sem, k, owner, lambda copy: copy.wait())

        @pl.when(k != own_k)
        def _():
            row_copy(k).wait_send()

        return c

    lax.fori_loop(0, group, finish, 0)


def first_kernel(group, waves, mom, grad, w_hbm, w_lo, w_hi, land, norms, send, norm_send, mom_v, grad_v, load_sem, m_send, m_recv,
                 n_send, n_recv, l_sem, *work):
    me = lax.axis_index("data")
    chips = group // CORES
    own_k = group - CORES
    rows_dev, cols = mom.shape[1:]
    steps = waves * group
    greet_group(me, group, chips)
    _, _, _, _, _, w_vmem, _, _, _, _, w_sem, _ = work
    mine = aligned(me * rows_dev, rows_dev)

    def block_of(t):
        return t // group, lax.rem(lax.rem(t, group) * (group // 2 + 1), group)

    def loads(t):
        wave, k = block_of(t)
        mat = wave * group + target_of(me, k, chips)
        slot = lax.rem(t, 2)
        return (
            pltpu.make_async_copy(mom.at[mat], mom_v.at[slot], load_sem.at[0, slot]),
            pltpu.make_async_copy(grad.at[mat], grad_v.at[slot], load_sem.at[1, slot]),
        )

    def remote(wave, k):
        target = target_of(me, k, chips)
        t = wave * group + k
        rows = pltpu.make_async_remote_copy(
            src_ref=send.at[t], dst_ref=land.at[wave, mine], send_sem=m_send.at[wave, k], recv_sem=m_recv.at[wave, k],
            device_id={"data": target}, device_id_type=MESH)
        norm = pltpu.make_async_remote_copy(
            src_ref=norm_send.at[t], dst_ref=norms.at[wave, me], send_sem=n_send.at[wave, k], recv_sem=n_recv.at[wave, k],
            device_id={"data": target}, device_id_type=MESH)
        return rows, norm

    def local(wave):
        t = wave * group + own_k
        return (
            pltpu.make_async_copy(send.at[t], land.at[wave, mine], l_sem.at[0, wave]),
            pltpu.make_async_copy(norm_send.at[t], norms.at[wave, me], l_sem.at[1, wave]),
        )

    def dispatch(t):
        wave, k = block_of(t)

        @pl.when(k == own_k)
        def _():
            for copy in local(wave):
                copy.start()

        @pl.when(k != own_k)
        def _():
            for copy in remote(wave, k):
                copy.start()

    for copy in loads(0):
        copy.start()

    def form(t, c):
        @pl.when(t + 1 < steps)
        def _():
            for copy in loads(t + 1):
                copy.start()

        for copy in loads(t):
            copy.wait()
        slot = lax.rem(t, 2)
        wave, k = block_of(t)
        at_send = wave * group + k

        def chunk(i, acc):
            at = aligned(i * CHUNK, CHUNK)
            new = MOMENTUM * mom_v[slot, at, :] + grad_v[slot, at, :].astype(F32)
            send[at_send, at, :] = new.astype(BF16)
            sq = new * new
            for r in range(0, CHUNK, 8):
                acc = acc + sq[r:r + 8, :]
            return acc

        acc = lax.fori_loop(0, rows_dev // CHUNK, chunk, jnp.zeros((8, cols), F32))
        part = acc[:, 0:128]
        for col in range(128, cols, 128):
            part = part + acc[:, col:col + 128]
        norm_send[at_send] = part

        @pl.when(t > 0)
        def _():
            dispatch(t - 1)

        return c

    lax.fori_loop(0, steps, form, 0)
    start_weights(me, 0, group, w_hbm, w_vmem, w_sem, chips)

    def arrived(wave):
        for k in range(group):
            if k != own_k:
                for copy in remote(wave, k):
                    copy.wait_recv()
        for copy in local(wave):
            copy.wait()

    arrived(0)
    orthogonalize_wave(me, 0, group, chips, land, norms, w_hbm, w_lo, w_hi, *work, then=lambda: dispatch(jnp.int32(steps - 1)))
    for wave in range(1, waves):
        arrived(wave)
    for wave in range(waves):
        for k in range(group):
            if k != own_k:
                for copy in remote(wave, k):
                    copy.wait_send()


def later_kernel(group, wave, land, norms, *refs):
    me = lax.axis_index("data")
    chips = group // CORES
    outs, (y, gram, poly, norm_v, y_sem, o_sem) = refs[:group], refs[group:]
    rows_dev = y.shape[0] // group
    iterate(wave, land, norms, y, gram, poly, norm_v, y_sem)
    stores = [
        pltpu.make_async_copy(y.at[aligned(target_of(me, k, chips) * rows_dev, rows_dev)], outs[k], o_sem.at[k])
        for k in range(group)
    ]
    for copy in stores:
        copy.start()
    for copy in stores:
        copy.wait()


def update_kernel(group, wave, scale, *refs):
    me = lax.axis_index("data")
    chips = group // CORES
    blocks, (w_hbm, w_lo, w_hi, x_vmem, w_vmem, o_vmem, x_sem, w_sem, o_sem) = refs[:group], refs[group:]
    owners = [source_of(me, k, chips) for k in range(group)]
    loads = [
        (
            pltpu.make_async_copy(blocks[k], x_vmem.at[k], x_sem.at[k]),
            pltpu.make_async_copy(w_hbm.at[wave * group + owners[k]], w_vmem.at[k], w_sem.at[k]),
        )
        for k in range(group)
    ]
    for pair in loads:
        for copy in pair:
            copy.start()
    for k in range(group):
        for copy in loads[k]:
            copy.wait()
        new_rows(scale, w_vmem, x_vmem, o_vmem, k)
        store_rows(o_vmem, w_lo, w_hi, o_sem, k, owners[k], lambda copy: copy.start())
    for k in range(group):
        store_rows(o_vmem, w_lo, w_hi, o_sem, k, owners[k], lambda copy: copy.wait())


def momentum_kernel(mom, grad, _, out):
    out[...] = MOMENTUM * mom[...] + grad[...].astype(F32)


def place_kernel(group, wave, pieces, *refs):
    me = lax.axis_index("data")
    chips = group // CORES
    out, buf, in_sem, out_sem = refs[-4:]
    slots, rows_dev = buf.shape[:2]
    lag = slots // 2
    steps = [(p, first, o, dx, dc) for p, (first, count, dx, dc) in enumerate(pieces) for o in range(count)]

    def take(t):
        p, _, o, _, _ = steps[t]
        return pltpu.make_async_copy(refs[p].at[o], buf.at[t % slots], in_sem.at[t % slots])

    def put(t):
        _, first, o, dx, dc = steps[t]
        owner_rows = lax.rem(me // CORES + chips - dx, chips) * CORES + lax.rem(lax.rem(me, CORES) + dc, CORES)
        dst = out.at[wave * group + first + o, aligned(owner_rows * rows_dev, rows_dev)]
        return pltpu.make_async_copy(buf.at[t % slots], dst, out_sem.at[t % slots])

    for t in range(len(steps) + lag):
        if t < len(steps):
            if t >= slots:
                put(t - slots).wait()
            take(t).start()
        if t >= lag:
            take(t - lag).wait()
            put(t - lag).start()
    for t in range(max(len(steps) - slots, 0), len(steps)):
        put(t).wait()


def solution(mesh):
    group = mesh.shape["data"]
    chips = group // CORES
    half = group // 2
    row_spec = P("stage", "data", None)
    full_spec = P("stage", None, None)
    any_spec = pl.BlockSpec(memory_space=pl.ANY)

    def shift(block, dx, dc):
        pairs = [(d, (d // CORES + dx) % chips * CORES + (d % CORES + dc) % CORES) for d in range(group)]
        return lax.ppermute(block, "data", pairs)

    def local_step(w_rows, mom_rows, grad_rows):
        mats, rows_dev, cols = mom_rows.shape
        rows = rows_dev * group
        waves = mats // group
        ns_flops = NS_ITERS * 2 * (2 * rows * cols * cols + cols**3)
        work = [
            pltpu.VMEM((rows, cols), BF16),
            pltpu.VMEM((cols, cols), BF16),
            pltpu.VMEM((cols, cols), BF16),
            pltpu.VMEM((group, 8, 128), F32),
            pltpu.VMEM((group, rows_dev, cols), BF16),
            pltpu.VMEM((group, rows_dev, cols), F32),
            pltpu.VMEM((group, rows_dev, cols), BF16),
            pltpu.SemaphoreType.DMA((2,)),
            pltpu.SemaphoreType.DMA((group,)),
            pltpu.SemaphoreType.DMA((group,)),
            pltpu.SemaphoreType.DMA((group,)),
            pltpu.SemaphoreType.DMA((group,)),
        ]
        half_shape = jax.ShapeDtypeStruct((half, rows_dev, cols), BF16)
        cost = pl.CostEstimate(flops=ns_flops, bytes_accessed=8 * rows * cols, transcendentals=0)

        def place(params, wave, pieces, after=None):
            blocks = [block for block, *_ in pieces]
            count = len(blocks)
            operands = blocks + [x for x in (params, after) if x is not None]
            return pl.pallas_call(
                functools.partial(place_kernel, group, wave, tuple(tuple(piece[1:]) for piece in pieces)),
                out_shape=jax.ShapeDtypeStruct((mats, rows, cols), BF16),
                in_specs=[any_spec] * len(operands),
                out_specs=any_spec,
                scratch_shapes=[
                    pltpu.VMEM((SLOTS, rows_dev, cols), BF16),
                    pltpu.SemaphoreType.DMA((SLOTS,)),
                    pltpu.SemaphoreType.DMA((SLOTS,)),
                ],
                input_output_aliases={count: 0} if params is not None else {},
                compiler_params=pltpu.CompilerParams(vmem_limit_bytes=VMEM_LIMIT),
                cost_estimate=pl.CostEstimate(
                    flops=count * half * rows_dev * cols * 40, bytes_accessed=4 * count * half * rows_dev * cols, transcendentals=0),
            )(*operands)

        w_lo, w_hi, land, norms = pl.pallas_call(
            functools.partial(first_kernel, group, waves),
            name="first_wave",
            out_shape=(
                half_shape,
                half_shape,
                jax.ShapeDtypeStruct((waves, rows, cols), BF16),
                jax.ShapeDtypeStruct((waves, group, 8, 128), F32),
            ),
            in_specs=[any_spec] * 3,
            out_specs=(any_spec,) * 4,
            scratch_shapes=[
                pltpu.VMEM((mats, rows_dev, cols), BF16),
                pltpu.VMEM((mats, 8, 128), F32),
                pltpu.VMEM((2, rows_dev, cols), F32),
                pltpu.VMEM((2, rows_dev, cols), BF16),
                pltpu.SemaphoreType.DMA((2, 2)),
                pltpu.SemaphoreType.DMA((waves, group)),
                pltpu.SemaphoreType.DMA((waves, group)),
                pltpu.SemaphoreType.DMA((waves, group)),
                pltpu.SemaphoreType.DMA((waves, group)),
                pltpu.SemaphoreType.DMA((2, waves)),
                *work,
            ],
            compiler_params=pltpu.CompilerParams(collective_id=0, has_side_effects=True, vmem_limit_bytes=VMEM_LIMIT),
            cost_estimate=cost,
        )(mom_rows, grad_rows, w_rows)

        def spread(lo, hi):
            up_lo, down_hi = shift(lo, 1, 0), shift(hi, chips - 1, 0)
            up_hi, down_lo = shift(hi, 1, 0), shift(lo, chips - 1, 0)
            return up_lo, down_lo, up_hi, down_hi

        def pass_on(near):
            return shift(near[0], 1, 0), shift(near[3], chips - 1, 0)

        def part_cores(block, first):
            count = block.shape[0]
            return (block, first, count, 2, 0), (shift(block, 0, 1), first, count, 2, 1)

        def both_cores(pair, dx):
            lo, hi = pair
            return [(lo, 0, half, dx, 0), (hi, half, half, dx, 0)], [
                (shift(lo, 0, 1), 0, half, dx, 1), (shift(hi, 0, 1), half, half, dx, 1)
            ]

        mom_after = w_lo
        own, near, far = [(w_lo, w_hi)], [spread(w_lo, w_hi)], []
        scale = 0.2 * math.sqrt(max(rows, cols))
        for wave in range(1, waves):
            x_rows = pl.pallas_call(
                functools.partial(later_kernel, group, wave),
                out_shape=(jax.ShapeDtypeStruct((rows_dev, cols), BF16),) * group,
                in_specs=[any_spec] * 2,
                out_specs=(any_spec,) * group,
                scratch_shapes=work[:4] + [pltpu.SemaphoreType.DMA((2,)), pltpu.SemaphoreType.DMA((group,))],
                compiler_params=pltpu.CompilerParams(vmem_limit_bytes=VMEM_LIMIT),
                cost_estimate=cost,
            )(land, norms)
            x_rows = [
                x_rows[k] if k == group - CORES else shift(x_rows[k], (k // CORES + 1) % chips, k % CORES)
                for k in range(group)
            ]
            w_lo, w_hi = pl.pallas_call(
                functools.partial(update_kernel, group, wave, scale),
                out_shape=(half_shape, half_shape),
                in_specs=[any_spec] * (group + 1),
                out_specs=(any_spec,) * 2,
                scratch_shapes=work[4:7] + [pltpu.SemaphoreType.DMA((group,))] * 3,
                compiler_params=pltpu.CompilerParams(vmem_limit_bytes=VMEM_LIMIT),
                cost_estimate=pl.CostEstimate(flops=rows * cols * 400, bytes_accessed=8 * rows * cols, transcendentals=0),
            )(*x_rows, w_rows)
            far.append(pass_on(near[-1]))
            own.append((w_lo, w_hi))
            near.append(spread(w_lo, w_hi))
        mom_new = pl.pallas_call(
            momentum_kernel,
            name="momentum",
            grid=(mats,),
            out_shape=jax.ShapeDtypeStruct(mom_rows.shape, F32),
            in_specs=[
                pl.BlockSpec((1, rows_dev, cols), lambda i: (i, 0, 0)),
                pl.BlockSpec((1, rows_dev, cols), lambda i: (i, 0, 0)),
                any_spec,
            ],
            out_specs=pl.BlockSpec((1, rows_dev, cols), lambda i: (i, 0, 0)),
            compiler_params=pltpu.CompilerParams(vmem_limit_bytes=VMEM_LIMIT),
            cost_estimate=pl.CostEstimate(flops=mats * rows_dev * cols * 100, bytes_accessed=10 * mats * rows_dev * cols, transcendentals=0),
        )(mom_rows, grad_rows, mom_after)

        own_p = [both_cores(own[w], 0) for w in range(waves)]
        up_p = [both_cores(near[w][0::2], 1) for w in range(waves)]
        down_p = [both_cores(near[w][1::2], chips - 1) for w in range(waves)]
        far_p = [both_cores(far[w], 2) for w in range(waves - 1)]
        last = waves - 1
        params = None
        for w in range(last):
            params = place(params, w, sum(own_p[w], []))
            params = place(params, w, sum(up_p[w] + down_p[w], []))
            if w < last - 1:
                params = place(params, w, sum(far_p[w], []))
        params = place(params, last, sum(own_p[last], []))
        params = place(params, last - 1, sum(far_p[last - 1], []))
        params = place(params, last, sum(up_p[last] + down_p[last], []))
        first_part, last_part = [], []
        for block, dx, first in ((near[last][0], 1, 0), (near[last][3], chips - 1, half)):
            cut = half - 1
            for rows_of, at, part in ((block[:cut], first, first_part), (block[cut:], first + cut, last_part)):
                far_block = shift(rows_of, dx, 0)
                part.append(part_cores(far_block, at))
        params = place(params, last, [p for pair in first_part for p in pair])
        params = place(params, last, [pair[0] for pair in last_part])
        params = place(params, last, [pair[1] for pair in last_part])
        return params, mom_new

    return jax.shard_map(local_step, mesh=mesh, in_specs=(row_spec,) * 3, out_specs=(full_spec, row_spec), check_vma=False)
```

```python
import functools
import math

import jax
import jax.numpy as jnp
from jax import lax
from jax.experimental import pallas as pl
from jax.experimental.pallas import tpu as pltpu
from jax.sharding import PartitionSpec as P


NS_ITERS = 5
MOMENTUM = 0.95
LEARN_RATE = 0.02
WEIGHT_DECAY = 0.1
NORM_EPS = 1e-7
COEF_A = 3.4445
COEF_B = -4.7750
COEF_C = 2.0315

MESH = pl.DeviceIdType.MESH
CORES = 2
BLK = 256
CHUNK = 32
SLOTS = 8
LAST_ROWS = 32
VMEM_LIMIT = 67043328
F32 = jnp.float32
BF16 = jnp.bfloat16


def aligned(start, size):
    return pl.ds(pl.multiple_of(start, size), size)


def step_offsets(k, chips):
    return lax.rem(k // CORES + 1, chips), lax.rem(k, CORES)


def target_of(me, k, chips):
    dx, dc = step_offsets(k, chips)
    return lax.rem(me // CORES + dx, chips) * CORES + lax.rem(lax.rem(me, CORES) + dc, CORES)


def source_of(me, k, chips):
    dx, dc = step_offsets(k, chips)
    return lax.rem(me // CORES + chips - dx, chips) * CORES + lax.rem(lax.rem(me, CORES) + dc, CORES)


def greet_group(me, group, chips):
    for k in range(group):
        if k != group - CORES:
            pl.semaphore_signal(
                pltpu.get_barrier_semaphore(), inc=1, device_id={"data": target_of(me, k, chips)}, device_id_type=MESH)


def newton_schulz(y, gram, poly):
    rows, cols = y.shape

    def fill(target, i, block):
        target[i:i + BLK, i:] = block
        for at in range(i + BLK, cols, BLK):
            target[at:at + BLK, i:i + BLK] = block[:, at - i:at - i + BLK].T

    def iteration(_, carry):
        for i in range(0, cols, BLK):
            block = lax.dot_general(y[:, i:i + BLK], y[:, i:], (((0,), (0,)), ((), ())), preferred_element_type=F32)
            fill(gram, i, block.astype(BF16))
        for i in range(0, cols, BLK):
            square = jnp.dot(gram[i:i + BLK, :], gram[:, i:], preferred_element_type=F32)
            fill(poly, i, (COEF_B * gram[i:i + BLK, i:].astype(F32) + COEF_C * square).astype(BF16))

        def update_block(i, c):
            at = aligned(i * BLK, BLK)
            part = y[at, :]
            prod = jnp.dot(part, poly[...], preferred_element_type=F32)
            y[at, :] = (COEF_A * part.astype(F32) + prod).astype(BF16)
            return c

        lax.fori_loop(0, rows // BLK, update_block, 0)
        return carry

    lax.fori_loop(0, NS_ITERS, iteration, 0)


def start_weights(me, wave, group, w_hbm, w_vmem, w_sem, chips):
    def load(k, c):
        owner = source_of(me, k, chips)
        pltpu.make_async_copy(w_hbm.at[wave * group + owner], w_vmem.at[k], w_sem.at[k]).start()
        return c

    lax.fori_loop(0, group, load, 0)


def iterate(wave, land, norms, y, gram, poly, norm_v, y_sem):
    rows = y.shape[0]
    load_y = pltpu.make_async_copy(land.at[wave], y, y_sem.at[0])
    load_n = pltpu.make_async_copy(norms.at[wave], norm_v, y_sem.at[1])
    load_y.start()
    load_n.start()
    load_y.wait()
    load_n.wait()
    total = jnp.sum(jnp.sum(norm_v[...], axis=0), axis=(0, 1), keepdims=True)
    denom = jnp.sqrt(total) + NORM_EPS

    def normalise(i, c):
        at = aligned(i * CHUNK, CHUNK)
        y[at, :] = (y[at, :].astype(F32) / denom).astype(BF16)
        return c

    lax.fori_loop(0, rows // CHUNK, normalise, 0)
    newton_schulz(y, gram, poly)


def new_rows(scale, w_vmem, x_vmem, o_vmem, k):
    def chunk(i, c):
        at = aligned(i * CHUNK, CHUNK)
        w_old = w_vmem[k, at, :]
        ortho = x_vmem[k, at, :].astype(F32) * scale
        o_vmem[k, at, :] = (w_old - LEARN_RATE * (ortho + WEIGHT_DECAY * w_old)).astype(BF16)
        return c

    lax.fori_loop(0, w_vmem.shape[1] // CHUNK, chunk, 0)


def store_rows(o_vmem, w_lo, w_hi, o_sem, k, owner, act):
    half = w_lo.shape[0]

    @pl.when(owner < half)
    def _():
        act(pltpu.make_async_copy(o_vmem.at[k], w_lo.at[owner], o_sem.at[k]))

    @pl.when(owner >= half)
    def _():
        act(pltpu.make_async_copy(o_vmem.at[k], w_hi.at[owner - half], o_sem.at[k]))


def orthogonalize_wave(me, wave, group, chips, land, norms, w_hbm, w_lo, w_hi, y, gram, poly, norm_v, x_land, w_vmem, o_vmem,
                       y_sem, x_send, x_recv, w_sem, o_sem, then):
    rows, cols = y.shape
    rows_dev = rows // group
    own_k = group - CORES
    scale = 0.2 * math.sqrt(max(rows, cols))
    iterate(wave, land, norms, y, gram, poly, norm_v, y_sem)

    def row_copy(k):
        target = target_of(me, k, chips)
        return pltpu.make_async_remote_copy(
            src_ref=y.at[aligned(target * rows_dev, rows_dev)],
            dst_ref=x_land.at[k],
            send_sem=x_send.at[k],
            recv_sem=x_recv.at[k],
            device_id={"data": target},
            device_id_type=MESH,
        )

    for k in range(group):
        if k != own_k:
            row_copy(k).start()
    then()
    own = pltpu.make_async_copy(y.at[aligned(me * rows_dev, rows_dev)], x_land.at[own_k], y_sem.at[0])
    own.start()

    def update(j, c):
        k = lax.rem(j + own_k, group)
        owner = source_of(me, k, chips)
        pltpu.make_async_copy(w_hbm.at[wave * group + owner], w_vmem.at[k], w_sem.at[k]).wait()

        @pl.when(k == own_k)
        def _():
            own.wait()

        @pl.when(k != own_k)
        def _():
            row_copy(k).wait_recv()

        new_rows(scale, w_vmem, x_land, o_vmem, k)
        store_rows(o_vmem, w_lo, w_hi, o_sem, k, owner, lambda copy: copy.start())
        return c

    lax.fori_loop(0, group, update, 0)

    def finish(k, c):
        owner = source_of(me, k, chips)
        store_rows(o_vmem, w_lo, w_hi, o_sem, k, owner, lambda copy: copy.wait())

        @pl.when(k != own_k)
        def _():
            row_copy(k).wait_send()

        return c

    lax.fori_loop(0, group, finish, 0)


def first_kernel(group, waves, mom, grad, w_hbm, w_lo, w_hi, land, norms, send, norm_send, mom_v, grad_v, load_sem, m_send, m_recv,
                 n_send, n_recv, l_sem, *work):
    me = lax.axis_index("data")
    chips = group // CORES
    own_k = group - CORES
    rows_dev, cols = mom.shape[1:]
    steps = waves * group
    greet_group(me, group, chips)
    _, _, _, _, _, w_vmem, _, _, _, _, w_sem, _ = work
    mine = aligned(me * rows_dev, rows_dev)

    def block_of(t):
        return t // group, lax.rem(lax.rem(t, group) * (group // 2 + 1), group)

    def loads(t):
        wave, k = block_of(t)
        mat = wave * group + target_of(me, k, chips)
        slot = lax.rem(t, 2)
        return (
            pltpu.make_async_copy(mom.at[mat], mom_v.at[slot], load_sem.at[0, slot]),
            pltpu.make_async_copy(grad.at[mat], grad_v.at[slot], load_sem.at[1, slot]),
        )

    def remote(wave, k):
        target = target_of(me, k, chips)
        t = wave * group + k
        rows = pltpu.make_async_remote_copy(
            src_ref=send.at[t], dst_ref=land.at[wave, mine], send_sem=m_send.at[wave, k], recv_sem=m_recv.at[wave, k],
            device_id={"data": target}, device_id_type=MESH)
        norm = pltpu.make_async_remote_copy(
            src_ref=norm_send.at[t], dst_ref=norms.at[wave, me], send_sem=n_send.at[wave, k], recv_sem=n_recv.at[wave, k],
            device_id={"data": target}, device_id_type=MESH)
        return rows, norm

    def local(wave):
        t = wave * group + own_k
        return (
            pltpu.make_async_copy(send.at[t], land.at[wave, mine], l_sem.at[0, wave]),
            pltpu.make_async_copy(norm_send.at[t], norms.at[wave, me], l_sem.at[1, wave]),
        )

    def dispatch(t):
        wave, k = block_of(t)

        @pl.when(k == own_k)
        def _():
            for copy in local(wave):
                copy.start()

        @pl.when(k != own_k)
        def _():
            for copy in remote(wave, k):
                copy.start()

    for copy in loads(0):
        copy.start()

    def form(t):
        @pl.when(t + 1 < steps)
        def _():
            for copy in loads(t + 1):
                copy.start()

        for copy in loads(t):
            copy.wait()
        slot = lax.rem(t, 2)
        wave, k = block_of(t)
        at_send = wave * group + k

        def chunk(i, acc):
            at = aligned(i * CHUNK, CHUNK)
            new = MOMENTUM * mom_v[slot, at, :] + grad_v[slot, at, :].astype(F32)
            send[at_send, at, :] = new.astype(BF16)
            sq = new * new
            for r in range(0, CHUNK, 8):
                acc = acc + sq[r:r + 8, :]
            return acc

        acc = lax.fori_loop(0, rows_dev // CHUNK, chunk, jnp.zeros((8, cols), F32))
        part = acc[:, 0:128]
        for col in range(128, cols, 128):
            part = part + acc[:, col:col + 128]
        norm_send[at_send] = part

    def form_and_send(t, c):
        form(t)
        dispatch(t - 1)
        return c

    form(jnp.int32(0))
    pl.semaphore_wait(pltpu.get_barrier_semaphore(), group - 1)
    lax.fori_loop(1, steps, form_and_send, 0)
    start_weights(me, 0, group, w_hbm, w_vmem, w_sem, chips)

    def arrived(wave):
        for k in range(group):
            if k != own_k:
                for copy in remote(wave, k):
                    copy.wait_recv()
        for copy in local(wave):
            copy.wait()

    arrived(0)
    orthogonalize_wave(me, 0, group, chips, land, norms, w_hbm, w_lo, w_hi, *work, then=lambda: dispatch(jnp.int32(steps - 1)))
    for wave in range(1, waves):
        arrived(wave)
    for wave in range(waves):
        for k in range(group):
            if k != own_k:
                for copy in remote(wave, k):
                    copy.wait_send()


def later_kernel(group, wave, land, norms, *refs):
    me = lax.axis_index("data")
    chips = group // CORES
    outs, (y, gram, poly, norm_v, y_sem, o_sem) = refs[:group], refs[group:]
    rows_dev = y.shape[0] // group
    iterate(wave, land, norms, y, gram, poly, norm_v, y_sem)
    stores = [
        pltpu.make_async_copy(y.at[aligned(target_of(me, k, chips) * rows_dev, rows_dev)], outs[k], o_sem.at[k])
        for k in range(group)
    ]
    for copy in stores:
        copy.start()
    for copy in stores:
        copy.wait()


def update_kernel(group, wave, scale, *refs):
    me = lax.axis_index("data")
    chips = group // CORES
    blocks, (w_hbm, w_lo, w_hi, x_vmem, w_vmem, o_vmem, x_sem, w_sem, o_sem) = refs[:group], refs[group:]
    owners = [source_of(me, k, chips) for k in range(group)]
    loads = [
        (
            pltpu.make_async_copy(blocks[k], x_vmem.at[k], x_sem.at[k]),
            pltpu.make_async_copy(w_hbm.at[wave * group + owners[k]], w_vmem.at[k], w_sem.at[k]),
        )
        for k in range(group)
    ]
    for pair in loads:
        for copy in pair:
            copy.start()
    for k in range(group):
        for copy in loads[k]:
            copy.wait()
        new_rows(scale, w_vmem, x_vmem, o_vmem, k)
        store_rows(o_vmem, w_lo, w_hi, o_sem, k, owners[k], lambda copy: copy.start())
    for k in range(group):
        store_rows(o_vmem, w_lo, w_hi, o_sem, k, owners[k], lambda copy: copy.wait())


def momentum_kernel(mom, grad, _, out):
    out[...] = MOMENTUM * mom[...] + grad[...].astype(F32)


def place_kernel(group, wave, pieces, *refs):
    me = lax.axis_index("data")
    chips = group // CORES
    out, buf, in_sem, out_sem = refs[-4:]
    slots, rows_dev = buf.shape[:2]
    lag = slots // 2
    steps = [(p, first, o, dx, dc, row) for p, (first, dx, dc, row) in enumerate(pieces) for o in range(refs[p].shape[0])]

    def slot(t):
        return buf.at[t % slots, pl.ds(0, refs[steps[t][0]].shape[1])]

    def take(t):
        p, _, o, _, _, _ = steps[t]
        return pltpu.make_async_copy(refs[p].at[o], slot(t), in_sem.at[t % slots])

    def put(t):
        p, first, o, dx, dc, row = steps[t]
        owner_rows = lax.rem(me // CORES + chips - dx, chips) * CORES + lax.rem(lax.rem(me, CORES) + dc, CORES)
        dst = out.at[wave * group + first + o, pl.ds(pl.multiple_of(owner_rows * rows_dev + row, LAST_ROWS), refs[p].shape[1])]
        return pltpu.make_async_copy(slot(t), dst, out_sem.at[t % slots])

    for t in range(len(steps) + lag):
        if t < len(steps):
            if t >= slots:
                put(t - slots).wait()
            take(t).start()
        if t >= lag:
            take(t - lag).wait()
            put(t - lag).start()
    for t in range(max(len(steps) - slots, 0), len(steps)):
        put(t).wait()


def solution(mesh):
    group = mesh.shape["data"]
    chips = group // CORES
    half = group // 2
    row_spec = P("stage", "data", None)
    full_spec = P("stage", None, None)
    any_spec = pl.BlockSpec(memory_space=pl.ANY)

    def shift(block, dx, dc):
        pairs = [(d, (d // CORES + dx) % chips * CORES + (d % CORES + dc) % CORES) for d in range(group)]
        return lax.ppermute(block, "data", pairs)

    def local_step(w_rows, mom_rows, grad_rows):
        mats, rows_dev, cols = mom_rows.shape
        rows = rows_dev * group
        waves = mats // group
        ns_flops = NS_ITERS * 2 * (2 * rows * cols * cols + cols**3)
        work = [
            pltpu.VMEM((rows, cols), BF16),
            pltpu.VMEM((cols, cols), BF16),
            pltpu.VMEM((cols, cols), BF16),
            pltpu.VMEM((group, 8, 128), F32),
            pltpu.VMEM((group, rows_dev, cols), BF16),
            pltpu.VMEM((group, rows_dev, cols), F32),
            pltpu.VMEM((group, rows_dev, cols), BF16),
            pltpu.SemaphoreType.DMA((2,)),
            pltpu.SemaphoreType.DMA((group,)),
            pltpu.SemaphoreType.DMA((group,)),
            pltpu.SemaphoreType.DMA((group,)),
            pltpu.SemaphoreType.DMA((group,)),
        ]
        half_shape = jax.ShapeDtypeStruct((half, rows_dev, cols), BF16)
        cost = pl.CostEstimate(flops=ns_flops, bytes_accessed=8 * rows * cols, transcendentals=0)

        def place(params, wave, pieces, after=None):
            blocks = [block for block, *_ in pieces]
            count = len(blocks)
            operands = blocks + [x for x in (params, after) if x is not None]
            return pl.pallas_call(
                functools.partial(place_kernel, group, wave, tuple(tuple(piece[1:]) for piece in pieces)),
                out_shape=jax.ShapeDtypeStruct((mats, rows, cols), BF16),
                in_specs=[any_spec] * len(operands),
                out_specs=any_spec,
                scratch_shapes=[
                    pltpu.VMEM((SLOTS, rows_dev, cols), BF16),
                    pltpu.SemaphoreType.DMA((SLOTS,)),
                    pltpu.SemaphoreType.DMA((SLOTS,)),
                ],
                input_output_aliases={count: 0} if params is not None else {},
                compiler_params=pltpu.CompilerParams(vmem_limit_bytes=VMEM_LIMIT),
                cost_estimate=pl.CostEstimate(
                    flops=count * half * rows_dev * cols * 40, bytes_accessed=4 * count * half * rows_dev * cols, transcendentals=0),
            )(*operands)

        w_lo, w_hi, land, norms = pl.pallas_call(
            functools.partial(first_kernel, group, waves),
            name="first_wave",
            out_shape=(
                half_shape,
                half_shape,
                jax.ShapeDtypeStruct((waves, rows, cols), BF16),
                jax.ShapeDtypeStruct((waves, group, 8, 128), F32),
            ),
            in_specs=[any_spec] * 3,
            out_specs=(any_spec,) * 4,
            scratch_shapes=[
                pltpu.VMEM((mats, rows_dev, cols), BF16),
                pltpu.VMEM((mats, 8, 128), F32),
                pltpu.VMEM((2, rows_dev, cols), F32),
                pltpu.VMEM((2, rows_dev, cols), BF16),
                pltpu.SemaphoreType.DMA((2, 2)),
                pltpu.SemaphoreType.DMA((waves, group)),
                pltpu.SemaphoreType.DMA((waves, group)),
                pltpu.SemaphoreType.DMA((waves, group)),
                pltpu.SemaphoreType.DMA((waves, group)),
                pltpu.SemaphoreType.DMA((2, waves)),
                *work,
            ],
            compiler_params=pltpu.CompilerParams(collective_id=0, has_side_effects=True, vmem_limit_bytes=VMEM_LIMIT),
            cost_estimate=cost,
        )(mom_rows, grad_rows, w_rows)

        def spread(lo, hi):
            up_lo, down_hi = shift(lo, 1, 0), shift(hi, chips - 1, 0)
            up_hi, down_lo = shift(hi, 1, 0), shift(lo, chips - 1, 0)
            return up_lo, down_lo, up_hi, down_hi

        def pass_on(near):
            return shift(near[0], 1, 0), shift(near[3], chips - 1, 0)

        def both_cores(pair, dx):
            lo, hi = pair
            return [(lo, 0, dx, 0, 0), (hi, half, dx, 0, 0)], [
                (shift(lo, 0, 1), 0, dx, 1, 0), (shift(hi, 0, 1), half, dx, 1, 0)
            ]

        mom_after = w_lo
        own, near, far = [(w_lo, w_hi)], [spread(w_lo, w_hi)], []
        scale = 0.2 * math.sqrt(max(rows, cols))
        for wave in range(1, waves):
            x_rows = pl.pallas_call(
                functools.partial(later_kernel, group, wave),
                out_shape=(jax.ShapeDtypeStruct((rows_dev, cols), BF16),) * group,
                in_specs=[any_spec] * 2,
                out_specs=(any_spec,) * group,
                scratch_shapes=work[:4] + [pltpu.SemaphoreType.DMA((2,)), pltpu.SemaphoreType.DMA((group,))],
                compiler_params=pltpu.CompilerParams(vmem_limit_bytes=VMEM_LIMIT),
                cost_estimate=cost,
            )(land, norms)
            x_rows = [
                x_rows[k] if k == group - CORES else shift(x_rows[k], (k // CORES + 1) % chips, k % CORES)
                for k in range(group)
            ]
            w_lo, w_hi = pl.pallas_call(
                functools.partial(update_kernel, group, wave, scale),
                out_shape=(half_shape, half_shape),
                in_specs=[any_spec] * (group + 1),
                out_specs=(any_spec,) * 2,
                scratch_shapes=work[4:7] + [pltpu.SemaphoreType.DMA((group,))] * 3,
                compiler_params=pltpu.CompilerParams(vmem_limit_bytes=VMEM_LIMIT),
                cost_estimate=pl.CostEstimate(flops=rows * cols * 400, bytes_accessed=8 * rows * cols, transcendentals=0),
            )(*x_rows, w_rows)
            far.append(pass_on(near[-1]))
            own.append((w_lo, w_hi))
            near.append(spread(w_lo, w_hi))
        mom_new = pl.pallas_call(
            momentum_kernel,
            name="momentum",
            grid=(mats,),
            out_shape=jax.ShapeDtypeStruct(mom_rows.shape, F32),
            in_specs=[
                pl.BlockSpec((1, rows_dev, cols), lambda i: (i, 0, 0)),
                pl.BlockSpec((1, rows_dev, cols), lambda i: (i, 0, 0)),
                any_spec,
            ],
            out_specs=pl.BlockSpec((1, rows_dev, cols), lambda i: (i, 0, 0)),
            compiler_params=pltpu.CompilerParams(vmem_limit_bytes=VMEM_LIMIT),
            cost_estimate=pl.CostEstimate(flops=mats * rows_dev * cols * 100, bytes_accessed=10 * mats * rows_dev * cols, transcendentals=0),
        )(mom_rows, grad_rows, mom_after)

        own_p = [both_cores(own[w], 0) for w in range(waves)]
        up_p = [both_cores(near[w][0::2], 1) for w in range(waves)]
        down_p = [both_cores(near[w][1::2], chips - 1) for w in range(waves)]
        far_p = [both_cores(far[w], 2) for w in range(waves - 1)]
        last = waves - 1
        params = None
        for w in range(last):
            params = place(params, w, sum(own_p[w], []))
            params = place(params, w, sum(up_p[w] + down_p[w], []))
            if w < last - 1:
                params = place(params, w, sum(far_p[w], []))
        params = place(params, last, sum(own_p[last], []))
        params = place(params, last - 1, sum(far_p[last - 1], []))
        params = place(params, last, sum(up_p[last] + down_p[last], []))
        placed = {part: [] for part in "abcz"}
        for block, dx, first in ((near[last][0], 1, 0), (near[last][3], chips - 1, half)):
            cut, row = half - 1, rows_dev - LAST_ROWS
            pieces = [("a", block[:cut - 1], 0, "a"), ("b", block[cut - 1:cut], cut - 1, "b"), ("c", block[cut:, :row], cut, "z")]
            for part, rows_of, at, swapped_in in pieces:
                far_block = shift(rows_of, dx, 0)
                placed[part].append((far_block, first + at, 2, 0, 0))
                placed[swapped_in].append((shift(far_block, 0, 1), first + at, 2, 1, 0))
            rows_of = block[cut:, row:]
            placed["z"].append((shift(rows_of, dx, 0), first + cut, 2, 0, row))
            placed["z"].append((shift(rows_of, dx, 1), first + cut, 2, 1, row))
        for pieces in placed.values():
            params = place(params, last, pieces)
        return params, mom_new

    return jax.shard_map(local_step, mesh=mesh, in_specs=(row_spec,) * 3, out_specs=(full_spec, row_spec), check_vma=False)
```

```python
import functools
import math

import jax
import jax.numpy as jnp
from jax import lax
from jax.experimental import pallas as pl
from jax.experimental.pallas import tpu as pltpu
from jax.sharding import PartitionSpec as P


NS_ITERS = 5
MOMENTUM = 0.95
LEARN_RATE = 0.02
WEIGHT_DECAY = 0.1
NORM_EPS = 1e-7
COEF_A = 3.4445
COEF_B = -4.7750
COEF_C = 2.0315

CORES = 2
BLK = 256
CHUNK = 32
SLOTS = 8
LAST_ROWS = 32
VMEM_LIMIT = 67043328
F32 = jnp.float32
BF16 = jnp.bfloat16


def aligned(start, size):
    return pl.ds(pl.multiple_of(start, size), size)


def step_offsets(k, chips):
    return lax.rem(k // CORES + 1, chips), lax.rem(k, CORES)


def target_of(me, k, chips):
    dx, dc = step_offsets(k, chips)
    return lax.rem(me // CORES + dx, chips) * CORES + lax.rem(lax.rem(me, CORES) + dc, CORES)


def source_of(me, k, chips):
    dx, dc = step_offsets(k, chips)
    return lax.rem(me // CORES + chips - dx, chips) * CORES + lax.rem(lax.rem(me, CORES) + dc, CORES)


def newton_schulz(y, gram, poly):
    rows, cols = y.shape

    def fill(target, i, block):
        target[i:i + BLK, i:] = block
        for at in range(i + BLK, cols, BLK):
            target[at:at + BLK, i:i + BLK] = block[:, at - i:at - i + BLK].T

    def iteration(_, carry):
        for i in range(0, cols, BLK):
            block = lax.dot_general(y[:, i:i + BLK], y[:, i:], (((0,), (0,)), ((), ())), preferred_element_type=F32)
            fill(gram, i, block.astype(BF16))
        for i in range(0, cols, BLK):
            square = jnp.dot(gram[i:i + BLK, :], gram[:, i:], preferred_element_type=F32)
            fill(poly, i, (COEF_B * gram[i:i + BLK, i:].astype(F32) + COEF_C * square).astype(BF16))

        def update_block(i, c):
            at = aligned(i * BLK, BLK)
            part = y[at, :]
            prod = jnp.dot(part, poly[...], preferred_element_type=F32)
            y[at, :] = (COEF_A * part.astype(F32) + prod).astype(BF16)
            return c

        lax.fori_loop(0, rows // BLK, update_block, 0)
        return carry

    lax.fori_loop(0, NS_ITERS, iteration, 0)


def new_rows(scale, w_vmem, x_vmem, o_vmem, k):
    def chunk(i, c):
        at = aligned(i * CHUNK, CHUNK)
        w_old = w_vmem[k, at, :]
        ortho = x_vmem[k, at, :].astype(F32) * scale
        o_vmem[k, at, :] = (w_old - LEARN_RATE * (ortho + WEIGHT_DECAY * w_old)).astype(BF16)
        return c

    lax.fori_loop(0, w_vmem.shape[1] // CHUNK, chunk, 0)


def store_rows(o_vmem, w_lo, w_hi, o_sem, k, owner, act):
    half = w_lo.shape[0]

    @pl.when(owner < half)
    def _():
        act(pltpu.make_async_copy(o_vmem.at[k], w_lo.at[owner], o_sem.at[k]))

    @pl.when(owner >= half)
    def _():
        act(pltpu.make_async_copy(o_vmem.at[k], w_hi.at[owner - half], o_sem.at[k]))


def form_kernel(group, entries, earlier, mom, grad, *refs):
    me = lax.axis_index("data")
    chips = group // CORES
    count = len(entries)
    sums_in, outs = refs[:len(earlier)], refs[len(earlier):len(earlier) + count]
    sums_out, (mom_v, grad_v, send, load_sem, out_sem) = refs[len(earlier) + count:-5], refs[-5:]
    rows_dev, cols = mom.shape[1:]

    def loads(t):
        wave, k = entries[t]
        mat, slot = wave * group + target_of(me, k, chips), t % 2
        return (
            pltpu.make_async_copy(mom.at[mat], mom_v.at[slot], load_sem.at[0, slot]),
            pltpu.make_async_copy(grad.at[mat], grad_v.at[slot], load_sem.at[1, slot]),
        )

    for i, ks in enumerate(earlier):
        for at, k in enumerate(ks):
            sums_out[k][0] = sums_in[i][at]
    for copy in loads(0):
        copy.start()
    stores = [pltpu.make_async_copy(send.at[t], outs[t], out_sem.at[t]) for t in range(count)]
    for t, (wave, k) in enumerate(entries):
        if t + 1 < count:
            for copy in loads(t + 1):
                copy.start()
        for copy in loads(t):
            copy.wait()

        def chunk(i, acc, t=t):
            at = aligned(i * CHUNK, CHUNK)
            new = MOMENTUM * mom_v[t % 2, at, :] + grad_v[t % 2, at, :].astype(F32)
            send[t, at, :] = new.astype(BF16)
            sq = new * new
            for r in range(0, CHUNK, 8):
                acc = acc + sq[r:r + 8, :]
            return acc

        acc = lax.fori_loop(0, rows_dev // CHUNK, chunk, jnp.zeros((8, cols), F32))
        part = acc[:, 0:128]
        for col in range(128, cols, 128):
            part = part + acc[:, col:col + 128]
        if earlier:
            sums_out[k][wave] = part
        else:
            sums_out[0][t] = part
        stores[t].start()
    for copy in stores:
        copy.wait()


def iterate_kernel(group, wave, *refs):
    me = lax.axis_index("data")
    chips = group // CORES
    blocks, sums, outs, (y, gram, poly, in_sem, out_sem) = refs[:group], refs[group:2 * group], refs[2 * group:3 * group], refs[3 * group:]
    rows = y.shape[0]
    rows_dev = rows // group
    loads = [
        pltpu.make_async_copy(blocks[k], y.at[aligned(source_of(me, k, chips) * rows_dev, rows_dev)], in_sem.at[k])
        for k in range(group)
    ]
    for copy in loads:
        copy.start()
    total = sums[0][wave]
    for k in range(1, group):
        total = total + sums[k][wave]
    denom = jnp.sqrt(jnp.sum(total, axis=(0, 1), keepdims=True)) + NORM_EPS
    for copy in loads:
        copy.wait()

    def normalise(i, c):
        at = aligned(i * CHUNK, CHUNK)
        y[at, :] = (y[at, :].astype(F32) / denom).astype(BF16)
        return c

    lax.fori_loop(0, rows // CHUNK, normalise, 0)
    newton_schulz(y, gram, poly)
    stores = [
        pltpu.make_async_copy(y.at[aligned(target_of(me, k, chips) * rows_dev, rows_dev)], outs[k], out_sem.at[k])
        for k in range(group)
    ]
    for copy in stores:
        copy.start()
    for copy in stores:
        copy.wait()


def update_kernel(group, wave, scale, *refs):
    me = lax.axis_index("data")
    chips = group // CORES
    blocks, (w_hbm, w_lo, w_hi, x_vmem, w_vmem, o_vmem, x_sem, w_sem, o_sem) = refs[:group], refs[group:]
    owners = [source_of(me, k, chips) for k in range(group)]
    loads = [
        (
            pltpu.make_async_copy(blocks[k], x_vmem.at[k], x_sem.at[k]),
            pltpu.make_async_copy(w_hbm.at[wave * group + owners[k]], w_vmem.at[k], w_sem.at[k]),
        )
        for k in range(group)
    ]
    for pair in loads:
        for copy in pair:
            copy.start()
    for k in range(group):
        for copy in loads[k]:
            copy.wait()
        new_rows(scale, w_vmem, x_vmem, o_vmem, k)
        store_rows(o_vmem, w_lo, w_hi, o_sem, k, owners[k], lambda copy: copy.start())
    for k in range(group):
        store_rows(o_vmem, w_lo, w_hi, o_sem, k, owners[k], lambda copy: copy.wait())


def momentum_kernel(mom, grad, _, out):
    out[...] = MOMENTUM * mom[...] + grad[...].astype(F32)


def place_kernel(group, wave, pieces, *refs):
    me = lax.axis_index("data")
    chips = group // CORES
    out, buf, in_sem, out_sem = refs[-4:]
    slots, rows_dev = buf.shape[:2]
    lag = slots // 2
    steps = [(p, first, o, dx, dc, row) for p, (first, dx, dc, row) in enumerate(pieces) for o in range(refs[p].shape[0])]

    def slot(t):
        return buf.at[t % slots, pl.ds(0, refs[steps[t][0]].shape[1])]

    def take(t):
        p, _, o, _, _, _ = steps[t]
        return pltpu.make_async_copy(refs[p].at[o], slot(t), in_sem.at[t % slots])

    def put(t):
        p, first, o, dx, dc, row = steps[t]
        owner_rows = lax.rem(me // CORES + chips - dx, chips) * CORES + lax.rem(lax.rem(me, CORES) + dc, CORES)
        dst = out.at[wave * group + first + o, pl.ds(pl.multiple_of(owner_rows * rows_dev + row, LAST_ROWS), refs[p].shape[1])]
        return pltpu.make_async_copy(slot(t), dst, out_sem.at[t % slots])

    for t in range(len(steps) + lag):
        if t < len(steps):
            if t >= slots:
                put(t - slots).wait()
            take(t).start()
        if t >= lag:
            take(t - lag).wait()
            put(t - lag).start()
    for t in range(max(len(steps) - slots, 0), len(steps)):
        put(t).wait()


def solution(mesh):
    group = mesh.shape["data"]
    chips = group // CORES
    half = group // 2
    row_spec = P("stage", "data", None)
    full_spec = P("stage", None, None)
    any_spec = pl.BlockSpec(memory_space=pl.ANY)

    def shift(block, dx, dc):
        pairs = [(d, (d // CORES + dx) % chips * CORES + (d % CORES + dc) % CORES) for d in range(group)]
        return lax.ppermute(block, "data", pairs)

    def local_step(w_rows, mom_rows, grad_rows):
        mats, rows_dev, cols = mom_rows.shape
        rows = rows_dev * group
        waves = mats // group
        ns_flops = NS_ITERS * 2 * (2 * rows * cols * cols + cols**3)
        half_shape = jax.ShapeDtypeStruct((half, rows_dev, cols), BF16)
        cost = pl.CostEstimate(flops=ns_flops, bytes_accessed=8 * rows * cols, transcendentals=0)

        def place(params, wave, pieces, after=None):
            blocks = [block for block, *_ in pieces]
            count = len(blocks)
            operands = blocks + [x for x in (params, after) if x is not None]
            return pl.pallas_call(
                functools.partial(place_kernel, group, wave, tuple(tuple(piece[1:]) for piece in pieces)),
                out_shape=jax.ShapeDtypeStruct((mats, rows, cols), BF16),
                in_specs=[any_spec] * len(operands),
                out_specs=any_spec,
                scratch_shapes=[
                    pltpu.VMEM((SLOTS, rows_dev, cols), BF16),
                    pltpu.SemaphoreType.DMA((SLOTS,)),
                    pltpu.SemaphoreType.DMA((SLOTS,)),
                ],
                input_output_aliases={count: 0} if params is not None else {},
                compiler_params=pltpu.CompilerParams(vmem_limit_bytes=VMEM_LIMIT),
                cost_estimate=pl.CostEstimate(
                    flops=count * half * rows_dev * cols * 40, bytes_accessed=4 * count * half * rows_dev * cols, transcendentals=0),
            )(*operands)

        block_shape = jax.ShapeDtypeStruct((rows_dev, cols), BF16)
        vmem_spec = pl.BlockSpec(memory_space=pltpu.VMEM)
        own_k, first, second, third, _ = partners(group)

        def form(entries, earlier=(), sums=()):
            count = len(entries)
            sums_shape = [(waves, 8, 128)] * group if earlier else [(count, 8, 128)]
            outs = pl.pallas_call(
                functools.partial(form_kernel, group, entries, earlier),
                out_shape=(block_shape,) * count + tuple(jax.ShapeDtypeStruct(shape, F32) for shape in sums_shape),
                in_specs=[any_spec] * 2 + [vmem_spec] * len(sums),
                out_specs=(any_spec,) * count + (vmem_spec,) * len(sums_shape),
                scratch_shapes=[
                    pltpu.VMEM((2, rows_dev, cols), F32),
                    pltpu.VMEM((2, rows_dev, cols), BF16),
                    pltpu.VMEM((count, rows_dev, cols), BF16),
                    pltpu.SemaphoreType.DMA((2, 2)),
                    pltpu.SemaphoreType.DMA((count,)),
                ],
                compiler_params=pltpu.CompilerParams(vmem_limit_bytes=VMEM_LIMIT),
                cost_estimate=pl.CostEstimate(
                    flops=count * rows_dev * cols * 100, bytes_accessed=8 * count * rows_dev * cols, transcendentals=0),
            )(mom_rows, grad_rows, *sums)
            return dict(zip(entries, outs[:count])), outs[count:]

        def send(block, k):
            if k == own_k:
                return block
            return shift(block, (k // CORES + 1) % chips, k % CORES)

        formed_a, sums_a = form(tuple((0, k) for k in first))
        formed_b, sums_b = form(tuple((0, k) for k in second))
        formed_c, sums = form(
            tuple((w, k) for w in range(waves) for k in (() if w == 0 else first + second) + third), (first, second), (*sums_a, *sums_b))
        formed = {**formed_a, **formed_b, **formed_c}
        sums = [send(sums[k], k) for k in range(group)]
        scale = 0.2 * math.sqrt(max(rows, cols))

        def wave_rows(wave):
            blocks = [send(formed[wave, k], k) for k in range(group)]
            x_rows = pl.pallas_call(
                functools.partial(iterate_kernel, group, wave),
                out_shape=(block_shape,) * group,
                in_specs=[any_spec] * group + [vmem_spec] * group,
                out_specs=(any_spec,) * group,
                scratch_shapes=[
                    pltpu.VMEM((rows, cols), BF16),
                    pltpu.VMEM((cols, cols), BF16),
                    pltpu.VMEM((cols, cols), BF16),
                    pltpu.SemaphoreType.DMA((group,)),
                    pltpu.SemaphoreType.DMA((group,)),
                ],
                compiler_params=pltpu.CompilerParams(vmem_limit_bytes=VMEM_LIMIT),
                cost_estimate=cost,
            )(*blocks, *sums)
            ready = x_rows[own_k]
            x_rows = [send(x_rows[k], k) for k in range(group)]
            lo, hi = pl.pallas_call(
                functools.partial(update_kernel, group, wave, scale),
                out_shape=(half_shape, half_shape),
                in_specs=[any_spec] * (group + 1),
                out_specs=(any_spec,) * 2,
                scratch_shapes=[
                    pltpu.VMEM((group, rows_dev, cols), BF16),
                    pltpu.VMEM((group, rows_dev, cols), F32),
                    pltpu.VMEM((group, rows_dev, cols), BF16),
                ] + [pltpu.SemaphoreType.DMA((group,))] * 3,
                compiler_params=pltpu.CompilerParams(vmem_limit_bytes=VMEM_LIMIT),
                cost_estimate=pl.CostEstimate(flops=rows * cols * 400, bytes_accessed=8 * rows * cols, transcendentals=0),
            )(*x_rows, w_rows)
            return lo, hi, ready

        def spread(lo, hi):
            up_lo, down_hi = shift(lo, 1, 0), shift(hi, chips - 1, 0)
            up_hi, down_lo = shift(hi, 1, 0), shift(lo, chips - 1, 0)
            return up_lo, down_lo, up_hi, down_hi

        def pass_on(near):
            return shift(near[0], 1, 0), shift(near[3], chips - 1, 0)

        def both_cores(pair, dx):
            lo, hi = pair
            return [(lo, 0, dx, 0, 0), (hi, half, dx, 0, 0)], [
                (shift(lo, 0, 1), 0, dx, 1, 0), (shift(hi, 0, 1), half, dx, 1, 0)
            ]

        w_lo, w_hi, mom_after = wave_rows(0)
        own, near, far = [(w_lo, w_hi)], [spread(w_lo, w_hi)], []
        for wave in range(1, waves):
            w_lo, w_hi, _ = wave_rows(wave)
            far.append(pass_on(near[-1]))
            own.append((w_lo, w_hi))
            near.append(spread(w_lo, w_hi))
        mom_new = pl.pallas_call(
            momentum_kernel,
            name="mom",
            grid=(mats,),
            out_shape=jax.ShapeDtypeStruct(mom_rows.shape, F32),
            in_specs=[
                pl.BlockSpec((1, rows_dev, cols), lambda i: (i, 0, 0)),
                pl.BlockSpec((1, rows_dev, cols), lambda i: (i, 0, 0)),
                any_spec,
            ],
            out_specs=pl.BlockSpec((1, rows_dev, cols), lambda i: (i, 0, 0)),
            compiler_params=pltpu.CompilerParams(vmem_limit_bytes=VMEM_LIMIT),
            cost_estimate=pl.CostEstimate(flops=mats * rows_dev * cols * 100, bytes_accessed=10 * mats * rows_dev * cols, transcendentals=0),
        )(mom_rows, grad_rows, mom_after)

        own_p = [both_cores(own[w], 0) for w in range(waves)]
        up_p = [both_cores(near[w][0::2], 1) for w in range(waves)]
        down_p = [both_cores(near[w][1::2], chips - 1) for w in range(waves)]
        far_p = [both_cores(far[w], 2) for w in range(waves - 1)]
        last = waves - 1
        params = None
        for w in range(last):
            params = place(params, w, sum(own_p[w], []))
            params = place(params, w, sum(up_p[w] + down_p[w], []))
            if w < last - 1:
                params = place(params, w, sum(far_p[w], []))
        params = place(params, last, sum(own_p[last], []))
        params = place(params, last - 1, sum(far_p[last - 1], []))
        params = place(params, last, sum(up_p[last] + down_p[last], []))
        placed = {part: [] for part in "abcz"}
        for block, dx, first in ((near[last][0], 1, 0), (near[last][3], chips - 1, half)):
            cut, row = half - 1, rows_dev - LAST_ROWS
            pieces = [("a", block[:cut - 1], 0, "a"), ("b", block[cut - 1:cut], cut - 1, "b"), ("c", block[cut:, :row], cut, "z")]
            for part, rows_of, at, swapped_in in pieces:
                far_block = shift(rows_of, dx, 0)
                placed[part].append((far_block, first + at, 2, 0, 0))
                placed[swapped_in].append((shift(far_block, 0, 1), first + at, 2, 1, 0))
            rows_of = block[cut:, row:]
            placed["z"].append((shift(rows_of, dx, 0), first + cut, 2, 0, row))
            placed["z"].append((shift(rows_of, dx, 1), first + cut, 2, 1, row))
        for pieces in placed.values():
            params = place(params, last, pieces)
        return params, mom_new

    return jax.shard_map(local_step, mesh=mesh, in_specs=(row_spec,) * 3, out_specs=(full_spec, row_spec), check_vma=False)


def partners(group):
    own_k = group - CORES
    two_hops = tuple(range(CORES, own_k - CORES))
    first = (0, two_hops[0])
    second = two_hops[1:] + (own_k - CORES,) + tuple(k for k in range(own_k - 1, 0, -1) if k not in two_hops + (own_k - CORES,))
    return own_k, first, second, tuple(range(own_k, group)), two_hops
```
